8 devices in a mesh: data: 1 (over z), row: 2 (over y), col: 4 (over x, core).
Axes of the slice: x: 2, y: 2, z: 1, core: 2. Of those that a mesh axis runs over, the one named last changes fastest.
Arguments:
- tokens: bfloat16 [1024, 2048], P(('data', 'row', 'col'))
- expert_ids: int32 [1024, 8], P(('data', 'row', 'col'))
- gate_weights: float32 [1024, 8], P(('data', 'row', 'col'))
- w_in: bfloat16 [256, 2048, 512], P(('row', 'col'))
- w_out: bfloat16 [256, 512, 2048], P(('row', 'col'))
Outputs:
- output: bfloat16 [1024, 2048], P(('data', 'row', 'col'))
All inputs are finite; a program needn't handle non-finite values.
Results may differ from the reference program's by a relative error of at most 0.00450213.
Values are sent between devices in bfloat16 or wider.
A program may use at most 1 GiB of HBM per device.

```python
import jax
import jax.numpy as jnp
from jax import lax

D = 2048
FF = 512
EXPERTS = 256
TOP = 8
TOK_DEV = 128
ROW = 2
COL = 4
GROUP = ROW * COL
TOKENS = GROUP * TOK_DEV
CAP = TOKENS * TOP // EXPERTS
AVG_LOAD = TOK_DEV * TOP // EXPERTS


def draw_routing(base_key):
    key_split, key_device = jax.random.split(base_key)
    shuffled = jax.random.permutation(key_split, EXPERTS)
    hot_set = shuffled[: EXPERTS // 2]
    cold_set = shuffled[EXPERTS // 2:]

    def one_device(device_index):
        device_key = jax.random.fold_in(key_device, device_index)
        key_shift, key_order, key_rows = jax.random.split(device_key, 3)
        shift_by = jax.random.randint(key_shift, (EXPERTS // 2,), 0, AVG_LOAD + 1)
        shift_by = shift_by.at[0].set(AVG_LOAD)
        counts = jnp.zeros((EXPERTS,), jnp.int32)
        counts = counts.at[hot_set].set(AVG_LOAD + shift_by).at[cold_set].set(AVG_LOAD - shift_by)
        expert_order = jax.random.permutation(key_order, EXPERTS)
        run_end = jnp.cumsum(counts[expert_order])
        position = jnp.arange(TOK_DEV * TOP)
        run_index = jnp.searchsorted(run_end, position, side='right')
        id_table = expert_order[run_index].reshape(TOP, TOK_DEV).T
        row_order = jax.random.permutation(key_rows, TOK_DEV)
        return id_table[row_order]

    return lax.map(one_device, jnp.arange(GROUP)).reshape(TOKENS, TOP).astype(jnp.int32)


def setup_inputs(seed: int = 0, part: int = 0) -> dict:
    base_key = jax.random.key(seed)
    key_tok, key_ids, key_gate, key_in, key_out = jax.random.split(base_key, 5)
    tokens = jax.random.normal(jax.random.fold_in(key_tok, part), (TOKENS, D), jnp.float32)
    expert_ids = draw_routing(jax.random.fold_in(key_ids, part))
    gate_weights = jax.random.uniform(jax.random.fold_in(key_gate, part), (TOKENS, TOP), jnp.float32, 0.25, 1.25) * TOP ** -0.5
    w_in = jax.random.normal(key_in, (EXPERTS, D, FF), jnp.float32) * D ** -0.5
    w_out = jax.random.normal(key_out, (EXPERTS, FF, D), jnp.float32) * FF ** -0.5
    return {'tokens': tokens.astype(jnp.bfloat16), 'expert_ids': expert_ids, 'gate_weights': gate_weights, 'w_in': w_in.astype(jnp.bfloat16), 'w_out': w_out.astype(jnp.bfloat16)}


def reference(tokens, expert_ids, gate_weights, w_in, w_out):
    flat_ids = expert_ids.reshape(-1)
    pair_count = flat_ids.shape[0]
    sort_order = jnp.argsort(flat_ids, stable=True)
    counts = jnp.bincount(flat_ids, length=EXPERTS)
    starts = jnp.cumsum(counts) - counts
    sorted_rank = jnp.arange(pair_count) - starts[flat_ids[sort_order]]
    pair_rank = jnp.zeros((pair_count,), jnp.int32).at[sort_order].set(sorted_rank)
    slot_of_pair = jnp.where(pair_rank < CAP, flat_ids * CAP + pair_rank, EXPERTS * CAP)
    token_of_pair = jnp.arange(pair_count) // TOP
    slot_token = jnp.full((EXPERTS * CAP,), TOKENS, jnp.int32).at[slot_of_pair].set(token_of_pair, mode='drop')
    padded = jnp.concatenate([tokens, jnp.zeros((1, D), tokens.dtype)], axis=0)

    def expert_ffn(operands):
        rows_index, w_first, w_second = operands
        buffer = padded[rows_index]
        hidden = jax.nn.gelu(jnp.dot(buffer, w_first, preferred_element_type=jnp.float32)).astype(jnp.bfloat16)
        return jnp.dot(hidden, w_second, preferred_element_type=jnp.float32).astype(jnp.bfloat16)

    expert_out = lax.map(expert_ffn, (slot_token.reshape(EXPERTS, CAP), w_in, w_out))
    out_pad = jnp.concatenate([expert_out.reshape(EXPERTS * CAP, D), jnp.zeros((1, D), expert_out.dtype)], axis=0)

    def combine(operands):
        block_tok, block_slot, block_gate = operands
        gathered = out_pad[block_slot]
        weighted = jnp.einsum('tk,tkd->td', block_gate.astype(jnp.float32), gathered.astype(jnp.float32))
        return (block_tok.astype(jnp.float32) + weighted).astype(jnp.bfloat16)

    layer_out = lax.map(combine, (tokens.reshape(GROUP, TOK_DEV, D), slot_of_pair.reshape(GROUP, TOK_DEV, TOP), gate_weights.reshape(GROUP, TOK_DEV, TOP)))
    return layer_out.reshape(TOKENS, D)
```

```python
import jax
import jax.numpy as jnp
from jax import lax
from jax.experimental import pallas as pl
from jax.experimental.pallas import tpu as pltpu
from jax.sharding import PartitionSpec as P

GRID_AXES = ('row', 'col')
MESH = pl.DeviceIdType.MESH
F32 = jnp.float32
BF16 = jnp.bfloat16

DEV = 8
TOK = 128
TOP = 8
D = 2048
FF = 512
LE = 32
CAP = 32
ALL = DEV * TOK
SLOTS = LE * CAP
CW = 512
NC = D // CW
GE = 8
NG = LE // GE
PIECES = NC * NG
RING = 6
HALF = TOK // 2
BF16_MAX = 3.3895313892515355e38


def kernel(tokens, meta, w_in, w_out, out, tok, meta_all, pos_t, lhs, expand, sel, gsel, buf, hacc, hid, o_buf, part, core_in,
           x_in, y_in, z_in, ring, w_sem, t_sem, m_send, m_recv, a_send, a_recv, r_send, r_recv):
    y = lax.axis_index('row')
    col = lax.axis_index('col')
    x = col // 2
    k = col % 2
    g = y * 4 + col

    def place(dy, dx, dk):
        return (1 - y if dy else y), (1 - x if dx else x), (1 - k if dk else k)

    def dev(dy, dx, dk):
        yy, xx, kk = place(dy, dx, dk)
        return {'row': yy, 'col': xx * 2 + kk}

    def block(dy, dx, dk):
        yy, xx, kk = place(dy, dx, dk)
        return kk * 4 + yy * 2 + xx

    def rows(dy, dx, dk):
        return pl.ds(pl.multiple_of(block(dy, dx, dk) * TOK, TOK), TOK)

    def half_rows(dy, dx, dk, h):
        return pl.ds(pl.multiple_of(block(dy, dx, dk) * TOK + h * HALF, HALF), HALF)

    own = block(0, 0, 0)

    def tok_copy(c):
        return pltpu.make_async_copy(tokens.at[:, pl.ds(c * CW, CW)], tok.at[c, rows(0, 0, 0)], t_sem.at[c])

    for c in range(NC):
        tok_copy(c).start()

    def in_copy(p, slot):
        c, gr = p // NG, p % NG
        return pltpu.make_async_copy(
            w_in.at[pl.ds(gr * GE, GE), pl.ds(pl.multiple_of(c * CW, CW), CW), :], ring.at[slot], w_sem.at[slot])

    def out_copy(p, slot):
        c, gr = p // NG, p % NG
        return pltpu.make_async_copy(
            w_out.at[pl.ds(gr * GE, GE), :, pl.ds(pl.multiple_of(c * CW, CW), CW)], ring.at[slot], w_sem.at[slot])

    for p in range(RING):
        in_copy(p, p).start()

    def refill(p, slot):
        nxt = p + RING

        @pl.when(nxt < PIECES)
        def _():
            in_copy(nxt, slot).start()

        @pl.when(jnp.logical_and(nxt >= PIECES, nxt < 2 * PIECES))
        def _():
            out_copy(nxt - PIECES, slot).start()

    rel = [(dy, dx, dk) for dy in (0, 1) for dx in (0, 1) for dk in (0, 1)]
    barrier = pltpu.get_barrier_semaphore()
    for r in rel[1:]:
        pl.semaphore_signal(barrier, inc=1, device_id=dev(*r), device_id_type=MESH)
    pl.semaphore_wait(barrier, DEV - 1)

    def meta_copy(i, dst):
        return pltpu.make_async_remote_copy(meta, meta_all.at[dst], m_send.at[i], m_recv.at[i], device_id=dev(*rel[i]),
                                            device_id_type=MESH)

    for i in range(1, DEV):
        meta_copy(i, own).start()

    def a_copy(c, i, region, to):
        ref = tok.at[c, region]
        return pltpu.make_async_remote_copy(ref, ref, a_send.at[c, i], a_recv.at[c, i], device_id=dev(*to), device_id_type=MESH)

    A_SENT = [((0, 0, 0), None, (0, 0, 1)), ((0, 0, 0), None, (0, 1, 0)), ((0, 0, 0), None, (1, 0, 0)),
              ((0, 1, 0), None, (0, 0, 1)), ((0, 1, 0), 0, (1, 0, 0)), ((1, 0, 0), None, (0, 0, 1)),
              ((1, 0, 0), 1, (0, 1, 0)), ((1, 1, 0), None, (0, 0, 1))]
    A_GOT = [((0, 0, 1), None), ((0, 1, 0), None), ((1, 0, 0), None), ((0, 1, 1), None), ((1, 1, 0), 0), ((1, 0, 1), None),
             ((1, 1, 0), 1), ((1, 1, 1), None)]

    def region(where, h):
        return rows(*where) if h is None else half_rows(*where, h)

    def a_start(c, i):
        where, h, to = A_SENT[i]
        a_copy(c, i, region(where, h), to).start()

    def a_wait_send(c, i):
        where, h, to = A_SENT[i]
        a_copy(c, i, region(where, h), to).wait_send()

    def a_wait(c, i):
        where, h = A_GOT[i]
        a_copy(c, i, region(where, h), A_SENT[i][2]).wait_recv()

    def a_own(c):
        tok_copy(c).wait()
        for i in (1, 2, 0):
            a_start(c, i)

    def a_forward(c):
        a_wait(c, 1)
        a_start(c, 4)
        a_start(c, 3)
        a_wait(c, 2)
        a_start(c, 6)
        a_start(c, 5)

    def a_corner(c):
        a_wait(c, 4)
        a_wait(c, 6)
        a_start(c, 7)

    a_own(0)
    a_own(1)

    lane = lax.broadcasted_iota(jnp.int32, (TOK, SLOTS), 1)
    sub = lax.broadcasted_iota(jnp.int32, (TOK, SLOTS), 0)
    lane_expert = lax.shift_right_logical(lane, 5)
    for q in range(4):
        expand[q] = jnp.where(sub - LE * q == lane_expert, 1.0, 0.0).astype(BF16)
    hacc[...] = jnp.zeros_like(hacc)
    meta_all[own] = meta[...]

    for i in range(1, DEV):
        meta_copy(i, block(*rel[i])).wait_recv()

    eid = (g * LE + lax.broadcasted_iota(jnp.int32, (LE, 1), 0)).astype(F32)
    upper = jnp.where(lax.broadcasted_iota(jnp.int32, (TOK, TOK), 0) < lax.broadcasted_iota(jnp.int32, (TOK, TOK), 1), 1.0, 0.0)
    upper = upper.astype(BF16)
    before = jnp.zeros((LE, 1), F32)
    for gi in range(DEV):
        b = (gi % 2) * 4 + (gi // 4) * 2 + (gi % 4) // 2
        chose = jnp.zeros((LE, TOK), F32)
        gate = jnp.zeros((LE, TOK), F32)
        for j in range(TOP):
            hit = meta_all[b, j:j + 1, :] == eid
            chose = chose + jnp.where(hit, 1.0, 0.0)
            gate = gate + jnp.where(hit, meta_all[b, TOP + j:TOP + j + 1, :], 0.0)
        rank = jnp.dot(chose.astype(BF16), upper, preferred_element_type=F32) + before
        before = before + jnp.sum(chose, axis=1, keepdims=True)
        pos = jnp.where(jnp.logical_and(chose > 0.0, rank < float(CAP)), rank, -1.0)
        pos_t[:, b * TOK:(b + 1) * TOK] = pos
        high = jnp.minimum(gate, BF16_MAX).astype(BF16).astype(F32)
        rest = gate - high
        mid = rest.astype(BF16).astype(F32)
        low = rest - mid
        table = jnp.concatenate([pos, high, mid, low], axis=0)
        lhs[b * TOK:(b + 1) * TOK, :] = table.T.astype(BF16)

    slot_rank = lax.broadcasted_iota(jnp.int32, (CAP, ALL), 0).astype(F32)

    def sel_step(e, _):
        row = pos_t[pl.ds(e, 1), :]
        sel[pl.ds(pl.multiple_of(e * CAP, CAP), CAP), :] = jnp.where(row == slot_rank, 1.0, 0.0).astype(BF16)
        return 0

    lax.fori_loop(0, LE, sel_step, 0)

    a_forward(0)
    a_own(2)

    lane_rank = jnp.bitwise_and(lax.broadcasted_iota(jnp.int32, (TOK, SLOTS), 1), CAP - 1).astype(F32)

    def gate_step(b, _):
        rr = pl.ds(pl.multiple_of(b * TOK, TOK), TOK)
        table = lhs[rr, :]
        mine = jnp.dot(table, expand[0], preferred_element_type=F32) == lane_rank
        for q in range(3):
            val = jnp.dot(table, expand[q + 1], preferred_element_type=F32)
            gsel[q, rr, :] = jnp.where(mine, val, 0.0).astype(BF16)
        return 0

    lax.fori_loop(0, DEV, gate_step, 0)
    a_corner(0)

    def expert_rows(gr, i):
        return pl.ds(pl.multiple_of((gr * GE + i) * CAP, CAP), CAP)

    def first_chunk(c, _):
        for i in (0, 3, 5, 7):
            a_wait(c, i)

        def dispatch(mb, _):
            rr = pl.ds(pl.multiple_of(mb * 256, 256), 256)
            buf[rr, :] = jnp.dot(sel[rr, :], tok[c], preferred_element_type=F32).astype(BF16)
            return 0

        lax.fori_loop(0, SLOTS // 256, dispatch, 0)

        def group(gr, _):
            @pl.when(jnp.logical_and(gr == 1, c + 1 < NC))
            def _():
                a_forward(c + 1)

            @pl.when(jnp.logical_and(gr == 1, c + 3 < NC))
            def _():
                a_own(c + 3)

            @pl.when(jnp.logical_and(gr == 3, c + 1 < NC))
            def _():
                a_corner(c + 1)

            p = c * NG + gr
            slot = p % RING
            in_copy(p, slot).wait()
            for i in range(GE):
                rr = expert_rows(gr, i)
                hacc[rr, :] += jnp.dot(buf[rr, :], ring[slot, i], preferred_element_type=F32)
            refill(p, slot)
            return 0

        lax.fori_loop(0, NG, group, 0)
        return 0

    lax.fori_loop(0, NC, first_chunk, 0)

    def act(mb, _):
        rr = pl.ds(pl.multiple_of(mb * 128, 128), 128)
        hid[rr, :] = jax.nn.gelu(hacc[rr, :]).astype(BF16)
        return 0

    lax.fori_loop(0, SLOTS // 128, act, 0)

    def core_copy(c):
        src = part.at[c, pl.ds(pl.multiple_of((1 - k) * 4 * TOK, 4 * TOK), 4 * TOK)]
        return pltpu.make_async_remote_copy(src, core_in.at[c], r_send.at[c, 0], r_recv.at[c, 0], device_id=dev(0, 0, 1),
                                            device_id_type=MESH)

    def r_copy(c, i, where, h, dst, to):
        return pltpu.make_async_remote_copy(part.at[c, half_rows(*where, h)], dst, r_send.at[c, i], r_recv.at[c, i],
                                            device_id=dev(*to), device_id_type=MESH)

    def r_copies(c):
        return [r_copy(c, 1, (1, 1, 0), 0, x_in.at[c, 1], (0, 1, 0)),
                r_copy(c, 2, (1, 1, 0), 1, y_in.at[c, 1], (1, 0, 0)),
                r_copy(c, 3, (0, 1, 0), 0, x_in.at[c, 0], (0, 1, 0)),
                r_copy(c, 4, (1, 0, 0), 1, y_in.at[c, 0], (1, 0, 0)),
                r_copy(c, 5, (1, 0, 0), 0, z_in.at[c, 0], (1, 0, 0)),
                r_copy(c, 6, (0, 1, 0), 1, z_in.at[c, 1], (0, 1, 0))]

    def r_first(c):
        core_copy(c).wait_recv()
        base = k * 4 * TOK

        def add(i, _):
            rr = pl.ds(pl.multiple_of(base + i * TOK, TOK), TOK)
            part[c, rr, :] = part[c, rr, :] + core_in[c, pl.ds(pl.multiple_of(i * TOK, TOK), TOK), :]
            return 0

        lax.fori_loop(0, 4, add, 0)
        cs = r_copies(c)
        for i in range(4):
            cs[i].start()

    def r_second(c):
        cs = r_copies(c)
        cs[0].wait_recv()
        rr = half_rows(1, 0, 0, 0)
        part[c, rr, :] = part[c, rr, :] + x_in[c, 1]
        cs[4].start()
        cs[1].wait_recv()
        rr = half_rows(0, 1, 0, 1)
        part[c, rr, :] = part[c, rr, :] + y_in[c, 1]
        cs[5].start()

    def r_last(c):
        cs = r_copies(c)
        for i in range(2, 6):
            cs[i].wait_recv()
        for h, near in ((0, x_in), (1, y_in)):
            rr = half_rows(0, 0, 0, h)
            total = part[c, rr, :] + near[c, 0] + z_in[c, h]
            total = tok[c, rr, :].astype(F32) + total
            out[h * HALF:(h + 1) * HALF, pl.ds(pl.multiple_of(c * CW, CW), CW)] = total.astype(BF16)

    def second_chunk(c, _):
        def group(gr, _):
            @pl.when(jnp.logical_and(gr == 1, c >= 1))
            def _():
                r_first(c - 1)

            @pl.when(jnp.logical_and(gr == 3, c >= 2))
            def _():
                r_second(c - 2)

            p = PIECES + c * NG + gr
            slot = p % RING
            out_copy(p - PIECES, slot).wait()
            for i in range(GE):
                rr = expert_rows(gr, i)
                o_buf[rr, :] = jnp.dot(hid[rr, :], ring[slot, i], preferred_element_type=F32).astype(BF16)
            refill(p, slot)
            return 0

        lax.fori_loop(0, NG, group, 0)

        def combine(mb, _):
            rr = pl.ds(pl.multiple_of(mb * 256, 256), 256)
            o = o_buf[...]
            acc = jnp.dot(gsel[0, rr, :], o, preferred_element_type=F32)
            acc = acc + jnp.dot(gsel[1, rr, :], o, preferred_element_type=F32)
            acc = acc + jnp.dot(gsel[2, rr, :], o, preferred_element_type=F32)
            part[c, rr, :] = acc
            return 0

        lax.fori_loop(0, ALL // 256, combine, 0)
        core_copy(c).start()
        return 0

    lax.fori_loop(0, NC, second_chunk, 0)
    r_first(NC - 1)
    r_second(NC - 2)

    def finish(c, _):
        r_last(c)
        return 0

    lax.fori_loop(0, NC - 1, finish, 0)
    r_second(NC - 1)
    r_last(NC - 1)

    for i in range(1, DEV):
        meta_copy(i, own).wait_send()

    def drain(c, _):
        for i in range(8):
            a_wait_send(c, i)
        core_copy(c).wait_send()
        for cp in r_copies(c):
            cp.wait_send()
        return 0

    lax.fori_loop(0, NC, drain, 0)


def solution(mesh):
    def device_fn(tokens, expert_ids, gate_weights, w_in, w_out):
        meta = jnp.concatenate([expert_ids.astype(F32), gate_weights], axis=1).T
        dma = pltpu.SemaphoreType.DMA
        any_spec = pl.BlockSpec(memory_space=pl.ANY)
        vmem_spec = pl.BlockSpec(memory_space=pltpu.VMEM)
        return pl.pallas_call(
            kernel,
            out_shape=jax.ShapeDtypeStruct((TOK, D), BF16),
            in_specs=[any_spec, vmem_spec, any_spec, any_spec],
            out_specs=vmem_spec,
            scratch_shapes=[
                pltpu.VMEM((NC, ALL, CW), BF16),
                pltpu.VMEM((DEV, 2 * TOP, TOK), F32),
                pltpu.VMEM((LE, ALL), F32),
                pltpu.VMEM((ALL, TOK), BF16),
                pltpu.VMEM((4, TOK, SLOTS), BF16),
                pltpu.VMEM((SLOTS, ALL), BF16),
                pltpu.VMEM((3, ALL, SLOTS), BF16),
                pltpu.VMEM((SLOTS, CW), BF16),
                pltpu.VMEM((SLOTS, FF), F32),
                pltpu.VMEM((SLOTS, FF), BF16),
                pltpu.VMEM((SLOTS, CW), BF16),
                pltpu.VMEM((NC, ALL, CW), F32),
                pltpu.VMEM((NC, ALL // 2, CW), F32),
                pltpu.VMEM((NC, 2, HALF, CW), F32),
                pltpu.VMEM((NC, 2, HALF, CW), F32),
                pltpu.VMEM((NC, 2, HALF, CW), F32),
                pltpu.VMEM((RING, GE, 512, CW), BF16),
                dma((RING,)), dma((NC,)), dma((DEV,)), dma((DEV,)), dma((NC, 8)), dma((NC, 8)), dma((NC, 7)), dma((NC, 7)),
            ],
            compiler_params=pltpu.CompilerParams(collective_id=0, has_side_effects=True, vmem_limit_bytes=67043328),
            name='experts',
        )(tokens, meta, w_in, w_out)

    token_spec = P(('data', 'row', 'col'), None)
    expert_spec = P(GRID_AXES, None, None)
    return jax.shard_map(device_fn, mesh=mesh, in_specs=(token_spec, token_spec, token_spec, expert_spec, expert_spec),
                         out_specs=token_spec, check_vma=False)
```

```python
import jax
import jax.numpy as jnp
from jax import lax
from jax.experimental import pallas as pl
from jax.experimental.pallas import tpu as pltpu
from jax.sharding import PartitionSpec as P

GRID_AXES = ('row', 'col')
MESH = pl.DeviceIdType.MESH
F32 = jnp.float32
BF16 = jnp.bfloat16

DEV = 8
TOK = 128
TOP = 8
D = 2048
FF = 512
LE = 32
CAP = 32
ALL = DEV * TOK
SLOTS = LE * CAP
CW = 512
NC = D // CW
GE = 8
NG = LE // GE
PIECES = NC * NG
RING = 6
CW2 = 256
NC2 = D // CW2
HALF = TOK // 2
BF16_MAX = 3.3895313892515355e38


def kernel(tokens, ids, gates, w_in, w_out, out, tok, meta, meta_all, pos_t, lhs, expand, sel, gsel, buf, hacc, hid, o_buf, part, core_in,
           x_in, y_in, z_in, ring, w_sem, t_sem, m_send, m_recv, a_send, a_recv, r_send, r_recv):
    y = lax.axis_index('row')
    col = lax.axis_index('col')
    x = col // 2
    k = col % 2
    g = y * 4 + col

    def place(dy, dx, dk):
        return (1 - y if dy else y), (1 - x if dx else x), (1 - k if dk else k)

    def dev(dy, dx, dk):
        yy, xx, kk = place(dy, dx, dk)
        return {'row': yy, 'col': xx * 2 + kk}

    def block(dy, dx, dk):
        yy, xx, kk = place(dy, dx, dk)
        return kk * 4 + yy * 2 + xx

    def rows(dy, dx, dk):
        return pl.ds(pl.multiple_of(block(dy, dx, dk) * TOK, TOK), TOK)

    def half_rows(dy, dx, dk, h):
        return pl.ds(pl.multiple_of(block(dy, dx, dk) * TOK + h * HALF, HALF), HALF)

    own = block(0, 0, 0)

    def tok_copy(c):
        return pltpu.make_async_copy(tokens.at[:, pl.ds(c * CW, CW)], tok.at[c, rows(0, 0, 0)], t_sem.at[c])

    for c in range(NC):
        tok_copy(c).start()

    def in_copy(p, slot):
        c, gr = p // NG, p % NG
        return pltpu.make_async_copy(
            w_in.at[pl.ds(gr * GE, GE), pl.ds(pl.multiple_of(c * CW, CW), CW), :], ring.at[slot], w_sem.at[slot])

    def out_copy(p, slot):
        c, gr = p // NG, p % NG
        return pltpu.make_async_copy(
            w_out.at[pl.ds(gr * GE, GE), :, pl.ds(pl.multiple_of(c * CW, CW), CW)], ring.at[slot], w_sem.at[slot])

    for p in range(RING):
        in_copy(p, p).start()

    def refill(p, slot):
        nxt = p + RING

        @pl.when(nxt < PIECES)
        def _():
            in_copy(nxt, slot).start()

        @pl.when(jnp.logical_and(nxt >= PIECES, nxt < 2 * PIECES))
        def _():
            out_copy(nxt - PIECES, slot).start()

    meta[0:TOP, :] = ids[...].astype(F32)
    meta[TOP:2 * TOP, :] = gates[...]

    rel = [(dy, dx, dk) for dy in (0, 1) for dx in (0, 1) for dk in (0, 1)]
    barrier = pltpu.get_barrier_semaphore()
    for r in rel[1:]:
        pl.semaphore_signal(barrier, inc=1, device_id=dev(*r), device_id_type=MESH)
    pl.semaphore_wait(barrier, DEV - 1)

    def meta_copy(i, dst):
        return pltpu.make_async_remote_copy(meta, meta_all.at[dst], m_send.at[i], m_recv.at[i], device_id=dev(*rel[i]),
                                            device_id_type=MESH)

    for i in range(1, DEV):
        meta_copy(i, own).start()

    def a_copy(c, i, region, to):
        ref = tok.at[c, region]
        return pltpu.make_async_remote_copy(ref, ref, a_send.at[c, i], a_recv.at[c, i], device_id=dev(*to), device_id_type=MESH)

    A_SENT = [((0, 0, 0), None, (0, 0, 1)), ((0, 0, 0), None, (0, 1, 0)), ((0, 0, 0), None, (1, 0, 0)),
              ((0, 1, 0), None, (0, 0, 1)), ((0, 1, 0), 0, (1, 0, 0)), ((1, 0, 0), None, (0, 0, 1)),
              ((1, 0, 0), 1, (0, 1, 0)), ((1, 1, 0), None, (0, 0, 1))]
    A_GOT = [((0, 0, 1), None), ((0, 1, 0), None), ((1, 0, 0), None), ((0, 1, 1), None), ((1, 1, 0), 0), ((1, 0, 1), None),
             ((1, 1, 0), 1), ((1, 1, 1), None)]

    def region(where, h):
        return rows(*where) if h is None else half_rows(*where, h)

    def a_start(c, i):
        where, h, to = A_SENT[i]
        a_copy(c, i, region(where, h), to).start()

    def a_wait_send(c, i):
        where, h, to = A_SENT[i]
        a_copy(c, i, region(where, h), to).wait_send()

    def a_wait(c, i):
        where, h = A_GOT[i]
        a_copy(c, i, region(where, h), A_SENT[i][2]).wait_recv()

    def a_own(c):
        tok_copy(c).wait()
        for i in (1, 2, 0):
            a_start(c, i)

    def a_forward(c):
        a_wait(c, 1)
        a_start(c, 4)
        a_start(c, 3)
        a_wait(c, 2)
        a_start(c, 6)
        a_start(c, 5)

    def a_corner(c):
        a_wait(c, 4)
        a_wait(c, 6)
        a_start(c, 7)

    a_own(0)
    a_own(1)

    lane = lax.broadcasted_iota(jnp.int32, (TOK, SLOTS), 1)
    sub = lax.broadcasted_iota(jnp.int32, (TOK, SLOTS), 0)
    lane_expert = lax.shift_right_logical(lane, 5)
    for q in range(4):
        expand[q] = jnp.where(sub - LE * q == lane_expert, 1.0, 0.0).astype(BF16)
    hacc[...] = jnp.zeros_like(hacc)
    meta_all[own] = meta[...]

    for i in range(1, DEV):
        meta_copy(i, block(*rel[i])).wait_recv()

    eid = (g * LE + lax.broadcasted_iota(jnp.int32, (LE, 1), 0)).astype(F32)
    upper = jnp.where(lax.broadcasted_iota(jnp.int32, (TOK, TOK), 0) < lax.broadcasted_iota(jnp.int32, (TOK, TOK), 1), 1.0, 0.0)
    upper = upper.astype(BF16)
    before = jnp.zeros((LE, 1), F32)
    for gi in range(DEV):
        b = (gi % 2) * 4 + (gi // 4) * 2 + (gi % 4) // 2
        chose = jnp.zeros((LE, TOK), F32)
        gate = jnp.zeros((LE, TOK), F32)
        for j in range(TOP):
            hit = meta_all[b, j:j + 1, :] == eid
            chose = chose + jnp.where(hit, 1.0, 0.0)
            gate = gate + jnp.where(hit, meta_all[b, TOP + j:TOP + j + 1, :], 0.0)
        rank = jnp.dot(chose.astype(BF16), upper, preferred_element_type=F32) + before
        before = before + jnp.sum(chose, axis=1, keepdims=True)
        pos = jnp.where(jnp.logical_and(chose > 0.0, rank < float(CAP)), rank, -1.0)
        pos_t[:, b * TOK:(b + 1) * TOK] = pos
        high = jnp.minimum(gate, BF16_MAX).astype(BF16).astype(F32)
        rest = gate - high
        mid = rest.astype(BF16).astype(F32)
        low = rest - mid
        table = jnp.concatenate([pos, high, mid, low], axis=0)
        lhs[b * TOK:(b + 1) * TOK, :] = table.T.astype(BF16)

    a_forward(0)
    a_own(2)

    slot_rank = lax.broadcasted_iota(jnp.int32, (CAP, ALL), 0).astype(F32)

    def sel_step(e, _):
        row = pos_t[pl.ds(e, 1), :]
        sel[pl.ds(pl.multiple_of(e * CAP, CAP), CAP), :] = jnp.where(row == slot_rank, 1.0, 0.0).astype(BF16)
        return 0

    lax.fori_loop(0, LE, sel_step, 0)

    lane_rank = jnp.bitwise_and(lax.broadcasted_iota(jnp.int32, (TOK, SLOTS), 1), CAP - 1).astype(F32)

    def gate_step(b, _):
        rr = pl.ds(pl.multiple_of(b * TOK, TOK), TOK)
        table = lhs[rr, :]
        mine = jnp.dot(table, expand[0], preferred_element_type=F32) == lane_rank
        for q in range(3):
            val = jnp.dot(table, expand[q + 1], preferred_element_type=F32)
            gsel[q, rr, :] = jnp.where(mine, val, 0.0).astype(BF16)
        return 0

    lax.fori_loop(0, DEV // 2, gate_step, 0)
    a_forward(1)
    a_own(3)
    lax.fori_loop(DEV // 2, DEV, gate_step, 0)
    a_corner(0)

    def expert_rows(gr, i):
        return pl.ds(pl.multiple_of((gr * GE + i) * CAP, CAP), CAP)

    def first_chunk(c, _):
        for i in (0, 3, 5, 7):
            a_wait(c, i)

        def dispatch(mb, _):
            rr = pl.ds(pl.multiple_of(mb * 256, 256), 256)
            buf[rr, :] = jnp.dot(sel[rr, :], tok[c], preferred_element_type=F32).astype(BF16)
            return 0

        lax.fori_loop(0, SLOTS // 256, dispatch, 0)

        def group(gr, _):
            @pl.when(jnp.logical_and(gr == 1, c + 2 < NC))
            def _():
                a_forward(c + 2)

            @pl.when(jnp.logical_and(gr == 2, c + 1 < NC))
            def _():
                a_corner(c + 1)

            p = c * NG + gr
            slot = p % RING
            in_copy(p, slot).wait()
            for i in range(GE):
                rr = expert_rows(gr, i)
                hacc[rr, :] += jnp.dot(buf[rr, :], ring[slot, i], preferred_element_type=F32)
            refill(p, slot)
            return 0

        lax.fori_loop(0, NG, group, 0)
        return 0

    lax.fori_loop(0, NC, first_chunk, 0)

    def act(mb, _):
        rr = pl.ds(pl.multiple_of(mb * 128, 128), 128)
        hid[rr, :] = jax.nn.gelu(hacc[rr, :]).astype(BF16)
        return 0

    lax.fori_loop(0, SLOTS // 128, act, 0)

    def core_copy(c):
        src = part.at[c, pl.ds(pl.multiple_of((1 - k) * 4 * TOK, 4 * TOK), 4 * TOK)]
        return pltpu.make_async_remote_copy(src, core_in.at[c], r_send.at[c, 0], r_recv.at[c, 0], device_id=dev(0, 0, 1),
                                            device_id_type=MESH)

    R_SENT = [None, ((1, 1, 0), 0, 0, 1), ((1, 1, 0), 1, 1, 1), ((0, 1, 0), 0, 0, 0), ((1, 0, 0), 1, 1, 0),
              ((1, 0, 0), 0, 2, 0), ((0, 1, 0), 1, 2, 1)]
    R_TO = [None, (0, 1, 0), (1, 0, 0), (0, 1, 0), (1, 0, 0), (1, 0, 0), (0, 1, 0)]

    def r_copy(c, i):
        where, h, box, at = R_SENT[i]
        return pltpu.make_async_remote_copy(part.at[c, half_rows(*where, h)], (x_in, y_in, z_in)[box].at[c, at],
                                            r_send.at[c, i], r_recv.at[c, i], device_id=dev(*R_TO[i]), device_id_type=MESH)

    def r_first(c):
        core_copy(c).wait_recv()
        base = k * 4 * TOK

        def add(i, _):
            rr = pl.ds(pl.multiple_of(base + i * TOK, TOK), TOK)
            part[c, rr, :] = part[c, rr, :] + core_in[c, pl.ds(pl.multiple_of(i * TOK, TOK), TOK), :]
            return 0

        lax.fori_loop(0, 4, add, 0)
        for i in range(1, 5):
            r_copy(c, i).start()

    def r_second(c):
        r_copy(c, 1).wait_recv()
        rr = half_rows(1, 0, 0, 0)
        part[c, rr, :] = part[c, rr, :] + x_in[c, 1]
        r_copy(c, 5).start()
        r_copy(c, 2).wait_recv()
        rr = half_rows(0, 1, 0, 1)
        part[c, rr, :] = part[c, rr, :] + y_in[c, 1]
        r_copy(c, 6).start()

    def r_last(c):
        for i in range(3, 7):
            r_copy(c, i).wait_recv()
        wide = c // 2
        cols = pl.ds(pl.multiple_of((c % 2) * CW2, CW2), CW2)
        for h, near in ((0, x_in), (1, y_in)):
            rr = half_rows(0, 0, 0, h)
            total = part[c, rr, :] + near[c, 0] + z_in[c, h]
            total = tok[wide, rr, cols].astype(F32) + total
            out[h * HALF:(h + 1) * HALF, pl.ds(pl.multiple_of(c * CW2, CW2), CW2)] = total.astype(BF16)

    def second_chunk(c, _):
        wide = c // 2
        half = c % 2
        cols = pl.ds(pl.multiple_of(half * CW2, CW2), CW2)

        def group(gr, _):
            @pl.when(jnp.logical_and(gr == 2, c >= 1))
            def _():
                r_first(c - 1)

            @pl.when(jnp.logical_and(gr == 3, c >= 3))
            def _():
                r_second(c - 3)

            q = wide * NG + gr
            p = PIECES + q
            slot = p % RING

            @pl.when(half == 0)
            def _():
                out_copy(q, slot).wait()

            for i in range(GE):
                rr = expert_rows(gr, i)
                o_buf[rr, :] = jnp.dot(hid[rr, :], ring[slot, i, :, cols], preferred_element_type=F32).astype(BF16)

            @pl.when(half == 1)
            def _():
                refill(p, slot)

            return 0

        lax.fori_loop(0, NG, group, 0)

        def combine(mb, _):
            rr = pl.ds(pl.multiple_of(mb * 256, 256), 256)
            o = o_buf[...]
            acc = jnp.dot(gsel[0, rr, :], o, preferred_element_type=F32)
            acc = acc + jnp.dot(gsel[1, rr, :], o, preferred_element_type=F32)
            acc = acc + jnp.dot(gsel[2, rr, :], o, preferred_element_type=F32)
            part[c, rr, :] = acc
            return 0

        lax.fori_loop(2 * (1 - k), 2 * (1 - k) + 2, combine, 0)
        core_copy(c).start()
        lax.fori_loop(2 * k, 2 * k + 2, combine, 0)
        return 0

    lax.fori_loop(0, NC2, second_chunk, 0)
    r_first(NC2 - 1)
    r_second(NC2 - 3)

    def finish(c, _):
        r_last(c)
        return 0

    lax.fori_loop(0, NC2 - 4, finish, 0)
    r_second(NC2 - 2)
    r_last(NC2 - 4)
    r_second(NC2 - 1)
    lax.fori_loop(NC2 - 3, NC2, finish, 0)

    for i in range(1, DEV):
        meta_copy(i, own).wait_send()

    def drain(c, _):
        for i in range(8):
            a_wait_send(c, i)
        return 0

    def r_drain(c, _):
        core_copy(c).wait_send()
        for i in range(1, 7):
            r_copy(c, i).wait_send()
        return 0

    lax.fori_loop(0, NC, drain, 0)
    lax.fori_loop(0, NC2, r_drain, 0)


def solution(mesh):
    def device_fn(tokens, expert_ids, gate_weights, w_in, w_out):
        dma = pltpu.SemaphoreType.DMA
        any_spec = pl.BlockSpec(memory_space=pl.ANY)
        vmem_spec = pl.BlockSpec(memory_space=pltpu.VMEM)
        return pl.pallas_call(
            kernel,
            out_shape=jax.ShapeDtypeStruct((TOK, D), BF16),
            in_specs=[any_spec, vmem_spec, vmem_spec, any_spec, any_spec],
            out_specs=vmem_spec,
            scratch_shapes=[
                pltpu.VMEM((NC, ALL, CW), BF16),
                pltpu.VMEM((2 * TOP, TOK), F32),
                pltpu.VMEM((DEV, 2 * TOP, TOK), F32),
                pltpu.VMEM((LE, ALL), F32),
                pltpu.VMEM((ALL, TOK), BF16),
                pltpu.VMEM((4, TOK, SLOTS), BF16),
                pltpu.VMEM((SLOTS, ALL), BF16),
                pltpu.VMEM((3, ALL, SLOTS), BF16),
                pltpu.VMEM((SLOTS, CW), BF16),
                pltpu.VMEM((SLOTS, FF), F32),
                pltpu.VMEM((SLOTS, FF), BF16),
                pltpu.VMEM((SLOTS, CW2), BF16),
                pltpu.VMEM((NC2, ALL, CW2), F32),
                pltpu.VMEM((NC2, ALL // 2, CW2), F32),
                pltpu.VMEM((NC2, 2, HALF, CW2), F32),
                pltpu.VMEM((NC2, 2, HALF, CW2), F32),
                pltpu.VMEM((NC2, 2, HALF, CW2), F32),
                pltpu.VMEM((RING, GE, 512, CW), BF16),
                dma((RING,)), dma((NC,)), dma((DEV,)), dma((DEV,)), dma((NC, 8)), dma((NC, 8)), dma((NC2, 7)), dma((NC2, 7)),
            ],
            compiler_params=pltpu.CompilerParams(collective_id=0, has_side_effects=True, vmem_limit_bytes=67043328),
            name='experts',
        )(tokens, expert_ids.T, gate_weights.T, w_in, w_out)

    token_spec = P(('data', 'row', 'col'), None)
    expert_spec = P(GRID_AXES, None, None)
    return jax.shard_map(device_fn, mesh=mesh, in_specs=(token_spec, token_spec, token_spec, expert_spec, expert_spec),
                         out_specs=token_spec, check_vma=False)
```

```python
import jax
import jax.numpy as jnp
from jax import lax
from jax.experimental import pallas as pl
from jax.experimental.pallas import tpu as pltpu
from jax.sharding import PartitionSpec as P

GRID_AXES = ('row', 'col')
MESH = pl.DeviceIdType.MESH
F32 = jnp.float32
BF16 = jnp.bfloat16

DEV = 8
TOK = 128
TOP = 8
D = 2048
FF = 512
LE = 32
CAP = 32
ALL = DEV * TOK
SLOTS = LE * CAP
CW = 512
NC = D // CW
GE = 8
NG = LE // GE
PIECES = NC * NG * 2
RING = 18
CW2 = 256
NC2 = D // CW2
HALF = TOK // 2
BF16_MAX = 3.3895313892515355e38


def kernel(tokens, ids, gates, w_in, w_out, out, tok, meta, meta_all, gsel, hid, core_in, x_in, y_in, z_in, ring, w_sem, t_sem, m_send, m_recv, a_send, a_recv, r_send, r_recv):
    y = lax.axis_index('row')
    col = lax.axis_index('col')
    x = col // 2
    k = col % 2
    g = y * 4 + col

    def place(dy, dx, dk):
        return (1 - y if dy else y), (1 - x if dx else x), (1 - k if dk else k)

    def dev(dy, dx, dk):
        yy, xx, kk = place(dy, dx, dk)
        return {'row': yy, 'col': xx * 2 + kk}

    def block(dy, dx, dk):
        yy, xx, kk = place(dy, dx, dk)
        return kk * 4 + xx * 2 + yy

    def rows(dy, dx, dk):
        return pl.ds(pl.multiple_of(block(dy, dx, dk) * TOK, TOK), TOK)

    def half_rows(dy, dx, dk, h):
        return pl.ds(pl.multiple_of(block(dy, dx, dk) * TOK + h * HALF, HALF), HALF)

    own = block(0, 0, 0)

    def tok_copy(c):
        return pltpu.make_async_copy(tokens.at[:, pl.ds(c * CW, CW)], tok.at[c, rows(0, 0, 0)], t_sem.at[c])

    for c in range(NC):
        tok_copy(c).start()

    def in_copy(p, slot):
        c, gr, half = p // (2 * NG), (p // 2) % NG, p % 2
        return pltpu.make_async_copy(
            w_in.at[pl.ds(gr * GE, GE), pl.ds(pl.multiple_of(c * CW, CW), CW), pl.ds(pl.multiple_of(half * 256, 256), 256)],
            ring.at[slot], w_sem.at[slot])

    def out_copy(p, slot):
        c, gr = p // NG, p % NG
        return pltpu.make_async_copy(
            w_out.at[pl.ds(gr * GE, GE), :, pl.ds(pl.multiple_of(c * CW2, CW2), CW2)], ring.at[slot], w_sem.at[slot])

    for p in range(RING):
        in_copy(p, p).start()

    def refill(p, slot):
        nxt = p + RING

        @pl.when(nxt < PIECES)
        def _():
            in_copy(nxt, slot).start()

        @pl.when(jnp.logical_and(nxt >= PIECES, nxt < 2 * PIECES))
        def _():
            out_copy(nxt - PIECES, slot).start()

    meta[0:TOP, :] = ids[...].astype(F32)
    meta[TOP:2 * TOP, :] = gates[...]

    rel = [(dy, dx, dk) for dy in (0, 1) for dx in (0, 1) for dk in (0, 1)]
    barrier = pltpu.get_barrier_semaphore()
    for r in rel[1:]:
        pl.semaphore_signal(barrier, inc=1, device_id=dev(*r), device_id_type=MESH)
    pl.semaphore_wait(barrier, DEV - 1)

    def meta_copy(i, dst):
        return pltpu.make_async_remote_copy(meta, meta_all.at[dst], m_send.at[i], m_recv.at[i], device_id=dev(*rel[i]),
                                            device_id_type=MESH)

    for i in range(1, DEV):
        meta_copy(i, own).start()

    def a_copy(c, i, region, to):
        ref = tok.at[c, region]
        return pltpu.make_async_remote_copy(ref, ref, a_send.at[c, i], a_recv.at[c, i], device_id=dev(*to), device_id_type=MESH)

    A_SENT = [((0, 0, 0), None, (0, 0, 1)), ((0, 0, 0), None, (0, 1, 0)), ((0, 0, 0), None, (1, 0, 0)),
              ((0, 1, 0), None, (0, 0, 1)), ((0, 1, 0), 0, (1, 0, 0)), ((1, 0, 0), None, (0, 0, 1)),
              ((1, 0, 0), 1, (0, 1, 0)), ((1, 1, 0), None, (0, 0, 1))]
    A_GOT = [((0, 0, 1), None), ((0, 1, 0), None), ((1, 0, 0), None), ((0, 1, 1), None), ((1, 1, 0), 0), ((1, 0, 1), None),
             ((1, 1, 0), 1), ((1, 1, 1), None)]

    def region(where, h):
        return rows(*where) if h is None else half_rows(*where, h)

    def a_start(c, i):
        where, h, to = A_SENT[i]
        a_copy(c, i, region(where, h), to).start()

    def a_wait_send(c, i):
        where, h, to = A_SENT[i]
        a_copy(c, i, region(where, h), to).wait_send()

    def a_wait(c, i):
        where, h = A_GOT[i]
        a_copy(c, i, region(where, h), A_SENT[i][2]).wait_recv()

    def a_own(c):
        tok_copy(c).wait()
        for i in (1, 2, 0):
            a_start(c, i)

    def a_forward(c):
        a_wait(c, 1)
        a_start(c, 4)
        a_start(c, 3)
        a_wait(c, 2)
        a_start(c, 6)
        a_start(c, 5)

    def a_corner(c):
        a_wait(c, 4)
        a_wait(c, 6)
        a_start(c, 7)

    a_own(0)
    a_own(1)

    def expert_rows(gr, i):
        return pl.ds(pl.multiple_of((gr * GE + i) * CAP, CAP), CAP)

    def gather_and_first(pos_t, lhs, expand, sel, buf, hacc):
        lane = lax.broadcasted_iota(jnp.int32, (TOK, SLOTS), 1)
        sub = lax.broadcasted_iota(jnp.int32, (TOK, SLOTS), 0)
        lane_expert = lax.shift_right_logical(lane, 5)
        for q in range(4):
            expand[q] = jnp.where(sub - LE * q == lane_expert, 1.0, 0.0).astype(BF16)
        hacc[...] = jnp.zeros_like(hacc)
        meta_all[own] = meta[...]

        for i in range(1, DEV):
            meta_copy(i, block(*rel[i])).wait_recv()

        eid = (g * LE + lax.broadcasted_iota(jnp.int32, (LE, 1), 0)).astype(F32)
        upper = jnp.where(lax.broadcasted_iota(jnp.int32, (TOK, TOK), 0) < lax.broadcasted_iota(jnp.int32, (TOK, TOK), 1), 1.0, 0.0)
        upper = upper.astype(BF16)
        before = jnp.zeros((LE, 1), F32)
        for gi in range(DEV):
            b = (gi % 2) * 4 + ((gi % 4) // 2) * 2 + gi // 4
            chose = jnp.zeros((LE, TOK), F32)
            gate = jnp.zeros((LE, TOK), F32)
            for j in range(TOP):
                hit = meta_all[b, j:j + 1, :] == eid
                chose = chose + jnp.where(hit, 1.0, 0.0)
                gate = gate + jnp.where(hit, meta_all[b, TOP + j:TOP + j + 1, :], 0.0)
            rank = jnp.dot(chose.astype(BF16), upper, preferred_element_type=F32) + before
            before = before + jnp.sum(chose, axis=1, keepdims=True)
            pos = jnp.where(jnp.logical_and(chose > 0.0, rank < float(CAP)), rank, -1.0)
            pos_t[:, b * TOK:(b + 1) * TOK] = pos
            high = jnp.minimum(gate, BF16_MAX).astype(BF16).astype(F32)
            rest = gate - high
            mid = rest.astype(BF16).astype(F32)
            low = rest - mid
            table = jnp.concatenate([pos, high, mid, low], axis=0)
            lhs[b * TOK:(b + 1) * TOK, :] = table.T.astype(BF16)

        a_forward(0)
        a_own(2)

        slot_rank = lax.broadcasted_iota(jnp.int32, (CAP, ALL), 0).astype(F32)

        def sel_step(e, _):
            row = pos_t[pl.ds(e, 1), :]
            sel[pl.ds(pl.multiple_of(e * CAP, CAP), CAP), :] = jnp.where(row == slot_rank, 1.0, 0.0).astype(BF16)
            return 0

        lax.fori_loop(0, LE, sel_step, 0)

        lane_rank = jnp.bitwise_and(lax.broadcasted_iota(jnp.int32, (TOK, SLOTS), 1), CAP - 1).astype(F32)

        def gate_step(b, _):
            rr = pl.ds(pl.multiple_of(b * TOK, TOK), TOK)
            table = lhs[rr, :]
            mine = jnp.dot(table, expand[0], preferred_element_type=F32) == lane_rank
            for q in range(3):
                val = jnp.dot(table, expand[q + 1], preferred_element_type=F32)
                gsel[q, rr, :] = jnp.where(mine, val, 0.0).astype(BF16)
            return 0

        lax.fori_loop(0, DEV // 2, gate_step, 0)
        a_forward(1)
        a_own(3)
        lax.fori_loop(DEV // 2, DEV, gate_step, 0)
        a_corner(0)

        def first_chunk(c, _):
            for i in (0, 3, 5, 7):
                a_wait(c, i)

            def dispatch(mb, _):
                rr = pl.ds(pl.multiple_of(mb * 256, 256), 256)
                buf[rr, :] = jnp.dot(sel[rr, :], tok[c], preferred_element_type=F32).astype(BF16)
                return 0

            lax.fori_loop(0, SLOTS // 256, dispatch, 0)

            def group(gr, _):
                @pl.when(jnp.logical_and(gr == 1, c + 2 < NC))
                def _():
                    a_forward(c + 2)

                @pl.when(jnp.logical_and(gr == 2, c + 1 < NC))
                def _():
                    a_corner(c + 1)

                p = (c * NG + gr) * 2
                slot = p % RING
                in_copy(p, slot).wait()
                in_copy(p + 1, slot + 1).wait()
                for i in range(GE):
                    rr = expert_rows(gr, i)
                    for h in range(2):
                        hacc[rr, h * 256:(h + 1) * 256] += jnp.dot(buf[rr, :], ring[slot + h, i], preferred_element_type=F32)
                refill(p, slot)
                refill(p + 1, slot + 1)
                return 0

            lax.fori_loop(0, NG, group, 0)
            return 0

        lax.fori_loop(0, NC, first_chunk, 0)

        def act(mb, _):
            rr = pl.ds(pl.multiple_of(mb * 128, 128), 128)
            hid[rr, :] = jax.nn.gelu(hacc[rr, :]).astype(BF16)
            return 0

        lax.fori_loop(0, SLOTS // 128, act, 0)

    pl.run_scoped(gather_and_first, pltpu.VMEM((LE, ALL), F32), pltpu.VMEM((ALL, TOK), BF16), pltpu.VMEM((4, TOK, SLOTS), BF16),
                  pltpu.VMEM((SLOTS, ALL), BF16), pltpu.VMEM((SLOTS, CW), BF16), pltpu.VMEM((SLOTS, FF), F32))

    def second_and_scatter(o_buf, part):
        def r_copy(c, i):
            src, dst, to = (
                (part.at[c, 1 - k], core_in.at[c], (0, 0, 1)),
                (part.at[c, k, 1 - x, :, 0], x_in.at[c], (0, 1, 0)),
                (part.at[c, k, :, 1 - y, 1], y_in.at[c], (1, 0, 0)),
                (part.at[c, k, x, 1 - y, 0], z_in.at[c, 0], (1, 0, 0)),
                (part.at[c, k, 1 - x, y, 1], z_in.at[c, 1], (0, 1, 0)),
            )[i]
            return pltpu.make_async_remote_copy(src, dst, r_send.at[c, i], r_recv.at[c, i], device_id=dev(*to), device_id_type=MESH)

        def r_first(c):
            r_copy(c, 0).wait_recv()

            def add(i, _):
                part[c, k, i] = part[c, k, i] + core_in[c, i]
                return 0

            lax.fori_loop(0, 2, add, 0)
            r_copy(c, 1).start()
            r_copy(c, 2).start()

        def r_second(c):
            r_copy(c, 1).wait_recv()
            part[c, k, x, 1 - y, 0] = part[c, k, x, 1 - y, 0] + x_in[c, 1 - y]
            r_copy(c, 3).start()
            r_copy(c, 2).wait_recv()
            part[c, k, 1 - x, y, 1] = part[c, k, 1 - x, y, 1] + y_in[c, 1 - x]
            r_copy(c, 4).start()

        def r_last(c):
            r_copy(c, 3).wait_recv()
            r_copy(c, 4).wait_recv()
            wide = c // 2
            cols = pl.ds(pl.multiple_of((c % 2) * CW2, CW2), CW2)
            for h in (0, 1):
                near = x_in[c, y] if h == 0 else y_in[c, x]
                total = part[c, k, x, y, h] + near + z_in[c, h]
                total = tok[wide, half_rows(0, 0, 0, h), cols].astype(F32) + total
                out[h * HALF:(h + 1) * HALF, pl.ds(pl.multiple_of(c * CW2, CW2), CW2)] = total.astype(BF16)

        def second_chunk(c, _):
            def group(gr, _):
                @pl.when(jnp.logical_and(gr == 1, c >= 3))
                def _():
                    r_second(c - 3)

                @pl.when(jnp.logical_and(gr == 3, c >= 1))
                def _():
                    r_first(c - 1)

                q = c * NG + gr
                p = PIECES + q
                slot = p % RING
                out_copy(q, slot).wait()
                for i in range(GE):
                    rr = expert_rows(gr, i)
                    o_buf[rr, :] = jnp.dot(hid[rr, :], ring[slot, i], preferred_element_type=F32).astype(BF16)
                refill(p, slot)
                return 0

            lax.fori_loop(0, NG, group, 0)

            def combine(mb, core):
                rr = pl.ds(pl.multiple_of(core * 512 + mb * 256, 256), 256)
                o = o_buf[...]
                acc = jnp.dot(gsel[0, rr, :], o, preferred_element_type=F32)
                acc = acc + jnp.dot(gsel[1, rr, :], o, preferred_element_type=F32)
                acc = acc + jnp.dot(gsel[2, rr, :], o, preferred_element_type=F32)
                part[c, core, mb] = acc.reshape(2, 2, HALF, CW2)
                return core

            lax.fori_loop(0, 2, combine, 1 - k)
            r_copy(c, 0).start()
            lax.fori_loop(0, 2, combine, k)
            return 0

        lax.fori_loop(0, NC2, second_chunk, 0)
        r_first(NC2 - 1)
        r_second(NC2 - 3)

        def finish(c, _):
            r_last(c)
            return 0

        lax.fori_loop(0, NC2 - 4, finish, 0)
        r_second(NC2 - 2)
        r_last(NC2 - 4)
        r_second(NC2 - 1)
        lax.fori_loop(NC2 - 3, NC2, finish, 0)

        def r_drain(c, _):
            for i in range(5):
                r_copy(c, i).wait_send()
            return 0

        lax.fori_loop(0, NC2, r_drain, 0)

    pl.run_scoped(second_and_scatter, pltpu.VMEM((SLOTS, CW2), BF16), pltpu.VMEM((NC2, 2, 2, 2, 2, HALF, CW2), F32))

    for i in range(1, DEV):
        meta_copy(i, own).wait_send()

    def drain(c, _):
        for i in range(8):
            a_wait_send(c, i)
        return 0

    lax.fori_loop(0, NC, drain, 0)


def solution(mesh):
    def device_fn(tokens, expert_ids, gate_weights, w_in, w_out):
        dma = pltpu.SemaphoreType.DMA
        any_spec = pl.BlockSpec(memory_space=pl.ANY)
        vmem_spec = pl.BlockSpec(memory_space=pltpu.VMEM)
        return pl.pallas_call(
            kernel,
            out_shape=jax.ShapeDtypeStruct((TOK, D), BF16),
            in_specs=[any_spec, vmem_spec, vmem_spec, any_spec, any_spec],
            out_specs=vmem_spec,
            scratch_shapes=[
                pltpu.VMEM((NC, ALL, CW), BF16),
                pltpu.VMEM((2 * TOP, TOK), F32),
                pltpu.VMEM((DEV, 2 * TOP, TOK), F32),
                pltpu.VMEM((3, ALL, SLOTS), BF16),
                pltpu.VMEM((SLOTS, FF), BF16),
                pltpu.VMEM((NC2, 2, 2, 2, HALF, CW2), F32),
                pltpu.VMEM((NC2, 2, HALF, CW2), F32),
                pltpu.VMEM((NC2, 2, HALF, CW2), F32),
                pltpu.VMEM((NC2, 2, HALF, CW2), F32),
                pltpu.VMEM((RING, GE, 512, 256), BF16),
                dma((RING,)), dma((NC,)), dma((DEV,)), dma((DEV,)), dma((NC, 8)), dma((NC, 8)), dma((NC2, 5)), dma((NC2, 5)),
            ],
            compiler_params=pltpu.CompilerParams(collective_id=0, has_side_effects=True, vmem_limit_bytes=67043328),
            name='experts',
        )(tokens, expert_ids.T, gate_weights.T, w_in, w_out)

    token_spec = P(('data', 'row', 'col'), None)
    expert_spec = P(GRID_AXES, None, None)
    return jax.shard_map(device_fn, mesh=mesh, in_specs=(token_spec, token_spec, token_spec, expert_spec, expert_spec),
                         out_specs=token_spec, check_vma=False)
```

```python
import jax
import jax.numpy as jnp
from jax import lax
from jax.experimental import pallas as pl
from jax.experimental.pallas import tpu as pltpu
from jax.sharding import PartitionSpec as P

GRID_AXES = ('row', 'col')
MESH = pl.DeviceIdType.MESH
F32 = jnp.float32
BF16 = jnp.bfloat16

DEV = 8
TOK = 128
TOP = 8
D = 2048
FF = 512
LE = 32
CAP = 32
ALL = DEV * TOK
SLOTS = LE * CAP
CW = 512
NC = D // CW
GE = 8
NG = LE // GE
PIECES = NC * NG * 2
RING = 18
CW2 = 256
NC2 = D // CW2
HALF = TOK // 2
BF16_MAX = 3.3895313892515355e38


def kernel(tokens, ids, gates, w_in, w_out, out, tok, meta, meta_all, gsel, hid, core_in, x_in, y_in, z_in, ring, w_sem, t_sem, m_send, m_recv, a_send, a_recv, r_send, r_recv):
    y = lax.axis_index('row')
    col = lax.axis_index('col')
    x = col // 2
    k = col % 2
    g = y * 4 + col

    def place(dy, dx, dk):
        return (1 - y if dy else y), (1 - x if dx else x), (1 - k if dk else k)

    def dev(dy, dx, dk):
        yy, xx, kk = place(dy, dx, dk)
        return {'row': yy, 'col': xx * 2 + kk}

    def block(dy, dx, dk):
        yy, xx, kk = place(dy, dx, dk)
        return kk * 4 + xx * 2 + yy

    def rows(dy, dx, dk):
        return pl.ds(pl.multiple_of(block(dy, dx, dk) * TOK, TOK), TOK)

    def half_rows(dy, dx, dk, h):
        return pl.ds(pl.multiple_of(block(dy, dx, dk) * TOK + h * HALF, HALF), HALF)

    own = block(0, 0, 0)

    def tok_copy(c):
        return pltpu.make_async_copy(tokens.at[:, pl.ds(c * CW, CW)], tok.at[c, rows(0, 0, 0)], t_sem.at[c])

    for c in range(NC):
        tok_copy(c).start()

    def in_copy(p, slot):
        c, gr, half = p // (2 * NG), (p // 2) % NG, p % 2
        return pltpu.make_async_copy(
            w_in.at[pl.ds(gr * GE, GE), pl.ds(pl.multiple_of(c * CW, CW), CW), pl.ds(pl.multiple_of(half * 256, 256), 256)],
            ring.at[slot], w_sem.at[slot])

    def out_copy(p, slot):
        c, gr = p // NG, p % NG
        return pltpu.make_async_copy(
            w_out.at[pl.ds(gr * GE, GE), :, pl.ds(pl.multiple_of(c * CW2, CW2), CW2)], ring.at[slot], w_sem.at[slot])

    for p in range(RING):
        in_copy(p, p).start()

    def refill(p, slot):
        nxt = p + RING

        @pl.when(nxt < PIECES)
        def _():
            in_copy(nxt, slot).start()

        @pl.when(jnp.logical_and(nxt >= PIECES, nxt < 2 * PIECES))
        def _():
            out_copy(nxt - PIECES, slot).start()

    meta[0:TOP, :] = ids[...].astype(F32)
    meta[TOP:2 * TOP, :] = gates[...]

    rel = [(dy, dx, dk) for dy in (0, 1) for dx in (0, 1) for dk in (0, 1)]
    barrier = pltpu.get_barrier_semaphore()
    for r in rel[1:]:
        pl.semaphore_signal(barrier, inc=1, device_id=dev(*r), device_id_type=MESH)
    pl.semaphore_wait(barrier, DEV - 1)

    def meta_copy(i, dst):
        return pltpu.make_async_remote_copy(meta, meta_all.at[dst], m_send.at[i], m_recv.at[i], device_id=dev(*rel[i]),
                                            device_id_type=MESH)

    for i in range(1, DEV):
        meta_copy(i, own).start()

    def a_copy(c, i, region, to):
        ref = tok.at[c, region]
        return pltpu.make_async_remote_copy(ref, ref, a_send.at[c, i], a_recv.at[c, i], device_id=dev(*to), device_id_type=MESH)

    A_SENT = [((0, 0, 0), None, (0, 0, 1)), ((0, 0, 0), None, (0, 1, 0)), ((0, 0, 0), None, (1, 0, 0)),
              ((0, 1, 0), None, (0, 0, 1)), ((0, 1, 0), 0, (1, 0, 0)), ((1, 0, 0), None, (0, 0, 1)),
              ((1, 0, 0), 1, (0, 1, 0)), ((1, 1, 0), None, (0, 0, 1))]
    A_GOT = [((0, 0, 1), None), ((0, 1, 0), None), ((1, 0, 0), None), ((0, 1, 1), None), ((1, 1, 0), 0), ((1, 0, 1), None),
             ((1, 1, 0), 1), ((1, 1, 1), None)]

    def region(where, h):
        return rows(*where) if h is None else half_rows(*where, h)

    def a_start(c, i):
        where, h, to = A_SENT[i]
        a_copy(c, i, region(where, h), to).start()

    def a_wait_send(c, i):
        where, h, to = A_SENT[i]
        a_copy(c, i, region(where, h), to).wait_send()

    def a_wait(c, i):
        where, h = A_GOT[i]
        a_copy(c, i, region(where, h), A_SENT[i][2]).wait_recv()

    def a_own(c):
        tok_copy(c).wait()
        for i in (1, 2, 0):
            a_start(c, i)

    def a_forward(c):
        a_wait(c, 1)
        a_start(c, 4)
        a_start(c, 3)
        a_wait(c, 2)
        a_start(c, 6)
        a_start(c, 5)

    def a_corner(c):
        a_wait(c, 4)
        a_wait(c, 6)
        a_start(c, 7)

    a_own(0)
    a_own(1)

    def expert_rows(gr, i):
        return pl.ds(pl.multiple_of((gr * GE + i) * CAP, CAP), CAP)

    def gather_and_first(pos_t, lhs, expand, sel, buf, hacc):
        lane = lax.broadcasted_iota(jnp.int32, (TOK, SLOTS), 1)
        sub = lax.broadcasted_iota(jnp.int32, (TOK, SLOTS), 0)
        lane_expert = lax.shift_right_logical(lane, 5)
        for q in range(4):
            expand[q] = jnp.where(sub - LE * q == lane_expert, 1.0, 0.0).astype(BF16)
        hacc[...] = jnp.zeros_like(hacc)
        meta_all[own] = meta[...]

        for i in range(1, DEV):
            meta_copy(i, block(*rel[i])).wait_recv()

        eid = (g * LE + lax.broadcasted_iota(jnp.int32, (LE, 1), 0)).astype(F32)
        upper = jnp.where(lax.broadcasted_iota(jnp.int32, (TOK, TOK), 0) < lax.broadcasted_iota(jnp.int32, (TOK, TOK), 1), 1.0, 0.0)
        upper = upper.astype(BF16)
        before = jnp.zeros((LE, 1), F32)
        for gi in range(DEV):
            b = (gi % 2) * 4 + ((gi % 4) // 2) * 2 + gi // 4
            chose = jnp.zeros((LE, TOK), F32)
            gate = jnp.zeros((LE, TOK), F32)
            for j in range(TOP):
                hit = meta_all[b, j:j + 1, :] == eid
                chose = chose + jnp.where(hit, 1.0, 0.0)
                gate = gate + jnp.where(hit, meta_all[b, TOP + j:TOP + j + 1, :], 0.0)
            rank = jnp.dot(chose.astype(BF16), upper, preferred_element_type=F32) + before
            before = before + jnp.sum(chose, axis=1, keepdims=True)
            pos = jnp.where(jnp.logical_and(chose > 0.0, rank < float(CAP)), rank, -1.0)
            pos_t[:, b * TOK:(b + 1) * TOK] = pos
            high = jnp.minimum(gate, BF16_MAX).astype(BF16).astype(F32)
            rest = gate - high
            mid = rest.astype(BF16).astype(F32)
            low = rest - mid
            table = jnp.concatenate([pos, high, mid, low], axis=0)
            lhs[b * TOK:(b + 1) * TOK, :] = table.T.astype(BF16)

        a_forward(0)
        a_own(2)

        slot_rank = lax.broadcasted_iota(jnp.int32, (CAP, ALL), 0).astype(F32)

        def sel_step(e, _):
            row = pos_t[pl.ds(e, 1), :]
            sel[pl.ds(pl.multiple_of(e * CAP, CAP), CAP), :] = jnp.where(row == slot_rank, 1.0, 0.0).astype(BF16)
            return 0

        lax.fori_loop(0, LE, sel_step, 0)

        lane_rank = jnp.bitwise_and(lax.broadcasted_iota(jnp.int32, (TOK, SLOTS), 1), CAP - 1).astype(F32)

        def gate_step(b, _):
            rr = pl.ds(pl.multiple_of(b * TOK, TOK), TOK)
            table = lhs[rr, :]
            mine = jnp.dot(table, expand[0], preferred_element_type=F32) == lane_rank
            for q in range(3):
                val = jnp.dot(table, expand[q + 1], preferred_element_type=F32)
                gsel[q, rr, :] = jnp.where(mine, val, 0.0).astype(BF16)
            return 0

        lax.fori_loop(0, DEV // 2, gate_step, 0)
        a_forward(1)
        a_own(3)
        lax.fori_loop(DEV // 2, DEV, gate_step, 0)
        a_corner(0)

        def first_chunk(c, _):
            for i in (0, 3, 5, 7):
                a_wait(c, i)

            for mb in range(2):
                buf[mb * 512:(mb + 1) * 512, :] = jnp.dot(sel[mb * 512:(mb + 1) * 512, :], tok[c],
                                                          preferred_element_type=F32).astype(BF16)

            def groups(gg, _):
                @pl.when(jnp.logical_and(gg == 0, c + 2 < NC))
                def _():
                    a_forward(c + 2)

                @pl.when(jnp.logical_and(gg == 1, c + 1 < NC))
                def _():
                    a_corner(c + 1)

                p = (c * NG + gg * 2) * 2
                for q in range(4):
                    in_copy(p + q, (p + q) % RING).wait()
                for u in range(2):
                    slot = (p + 2 * u) % RING
                    for i in range(GE):
                        rr = expert_rows(gg * 2 + u, i)
                        for h in range(2):
                            hacc[rr, h * 256:(h + 1) * 256] += jnp.dot(buf[rr, :], ring[slot + h, i], preferred_element_type=F32)
                for q in range(4):
                    refill(p + q, (p + q) % RING)
                return 0

            lax.fori_loop(0, NG // 2, groups, 0)
            return 0

        lax.fori_loop(0, NC, first_chunk, 0)

        def act(mb, _):
            rr = pl.ds(pl.multiple_of(mb * 128, 128), 128)
            hid[rr, :] = jax.nn.gelu(hacc[rr, :]).astype(BF16)
            return 0

        lax.fori_loop(0, SLOTS // 128, act, 0)

    pl.run_scoped(gather_and_first, pltpu.VMEM((LE, ALL), F32), pltpu.VMEM((ALL, TOK), BF16), pltpu.VMEM((4, TOK, SLOTS), BF16),
                  pltpu.VMEM((SLOTS, ALL), BF16), pltpu.VMEM((SLOTS, CW), BF16), pltpu.VMEM((SLOTS, FF), F32))

    def second_and_scatter(o_buf, part):
        def r_copy(c, i):
            src, dst, to = (
                (part.at[c, 1 - k], core_in.at[c], (0, 0, 1)),
                (part.at[c, k, 1 - x, :, 0], x_in.at[c], (0, 1, 0)),
                (part.at[c, k, :, 1 - y, 1], y_in.at[c], (1, 0, 0)),
                (part.at[c, k, x, 1 - y, 0], z_in.at[c, 0], (1, 0, 0)),
                (part.at[c, k, 1 - x, y, 1], z_in.at[c, 1], (0, 1, 0)),
            )[i]
            return pltpu.make_async_remote_copy(src, dst, r_send.at[c, i], r_recv.at[c, i], device_id=dev(*to), device_id_type=MESH)

        def r_first(c):
            r_copy(c, 0).wait_recv()

            def add(i, _):
                part[c, k, i] = part[c, k, i] + core_in[c, i]
                return 0

            lax.fori_loop(0, 2, add, 0)
            r_copy(c, 1).start()
            r_copy(c, 2).start()

        def r_second(c):
            r_copy(c, 1).wait_recv()
            part[c, k, x, 1 - y, 0] = part[c, k, x, 1 - y, 0] + x_in[c, 1 - y]
            r_copy(c, 3).start()
            r_copy(c, 2).wait_recv()
            part[c, k, 1 - x, y, 1] = part[c, k, 1 - x, y, 1] + y_in[c, 1 - x]
            r_copy(c, 4).start()

        def r_last(c):
            r_copy(c, 3).wait_recv()
            r_copy(c, 4).wait_recv()
            wide = c // 2
            cols = pl.ds(pl.multiple_of((c % 2) * CW2, CW2), CW2)
            for h in (0, 1):
                near = x_in[c, y] if h == 0 else y_in[c, x]
                total = part[c, k, x, y, h] + near + z_in[c, h]
                total = tok[wide, half_rows(0, 0, 0, h), cols].astype(F32) + total
                out[h * HALF:(h + 1) * HALF, pl.ds(pl.multiple_of(c * CW2, CW2), CW2)] = total.astype(BF16)

        def second_chunk(c, _):
            @pl.when(c >= 3)
            def _():
                r_second(c - 3)

            p = PIECES + c * NG
            for q in range(NG):
                out_copy(c * NG + q, (p + q) % RING).wait()
            for q in range(NG):
                slot = (p + q) % RING
                for i in range(GE):
                    e = q * GE + i
                    o_buf[e * CAP:(e + 1) * CAP, :] = jnp.dot(hid[e * CAP:(e + 1) * CAP, :], ring[slot, i],
                                                              preferred_element_type=F32).astype(BF16)
            for q in range(NG):
                refill(p + q, (p + q) % RING)

            @pl.when(c >= 1)
            def _():
                r_first(c - 1)

            def combine(core):
                rr = pl.ds(pl.multiple_of(core * 512, 512), 512)
                o = o_buf[...]
                acc = jnp.dot(gsel[0, rr, :], o, preferred_element_type=F32)
                acc = acc + jnp.dot(gsel[1, rr, :], o, preferred_element_type=F32)
                acc = acc + jnp.dot(gsel[2, rr, :], o, preferred_element_type=F32)
                part[c, core] = acc.reshape(2, 2, 2, HALF, CW2)

            combine(1 - k)
            r_copy(c, 0).start()
            combine(k)
            return 0

        lax.fori_loop(0, NC2, second_chunk, 0)
        r_first(NC2 - 1)
        r_second(NC2 - 3)

        def finish(c, _):
            r_last(c)
            return 0

        lax.fori_loop(0, NC2 - 4, finish, 0)
        r_second(NC2 - 2)
        r_last(NC2 - 4)
        r_second(NC2 - 1)
        lax.fori_loop(NC2 - 3, NC2, finish, 0)

        def r_drain(c, _):
            for i in range(5):
                r_copy(c, i).wait_send()
            return 0

        lax.fori_loop(0, NC2, r_drain, 0)

    pl.run_scoped(second_and_scatter, pltpu.VMEM((SLOTS, CW2), BF16), pltpu.VMEM((NC2, 2, 2, 2, 2, HALF, CW2), F32))

    for i in range(1, DEV):
        meta_copy(i, own).wait_send()

    def drain(c, _):
        for i in range(8):
            a_wait_send(c, i)
        return 0

    lax.fori_loop(0, NC, drain, 0)


def solution(mesh):
    def device_fn(tokens, expert_ids, gate_weights, w_in, w_out):
        dma = pltpu.SemaphoreType.DMA
        any_spec = pl.BlockSpec(memory_space=pl.ANY)
        vmem_spec = pl.BlockSpec(memory_space=pltpu.VMEM)
        return pl.pallas_call(
            kernel,
            out_shape=jax.ShapeDtypeStruct((TOK, D), BF16),
            in_specs=[any_spec, vmem_spec, vmem_spec, any_spec, any_spec],
            out_specs=vmem_spec,
            scratch_shapes=[
                pltpu.VMEM((NC, ALL, CW), BF16),
                pltpu.VMEM((2 * TOP, TOK), F32),
                pltpu.VMEM((DEV, 2 * TOP, TOK), F32),
                pltpu.VMEM((3, ALL, SLOTS), BF16),
                pltpu.VMEM((SLOTS, FF), BF16),
                pltpu.VMEM((NC2, 2, 2, 2, HALF, CW2), F32),
                pltpu.VMEM((NC2, 2, HALF, CW2), F32),
                pltpu.VMEM((NC2, 2, HALF, CW2), F32),
                pltpu.VMEM((NC2, 2, HALF, CW2), F32),
                pltpu.VMEM((RING, GE, 512, 256), BF16),
                dma((RING,)), dma((NC,)), dma((DEV,)), dma((DEV,)), dma((NC, 8)), dma((NC, 8)), dma((NC2, 5)), dma((NC2, 5)),
            ],
            compiler_params=pltpu.CompilerParams(collective_id=0, has_side_effects=True, vmem_limit_bytes=67043328),
            name='experts',
        )(tokens, expert_ids.T, gate_weights.T, w_in, w_out)

    token_spec = P(('data', 'row', 'col'), None)
    expert_spec = P(GRID_AXES, None, None)
    return jax.shard_map(device_fn, mesh=mesh, in_specs=(token_spec, token_spec, token_spec, expert_spec, expert_spec),
                         out_specs=token_spec, check_vma=False)
```

```python
import jax
import jax.numpy as jnp
from jax import lax
from jax.experimental import pallas as pl
from jax.experimental.pallas import tpu as pltpu
from jax.sharding import PartitionSpec as P

GRID_AXES = ('row', 'col')
MESH = pl.DeviceIdType.MESH
F32 = jnp.float32
BF16 = jnp.bfloat16

DEV = 8
TOK = 128
TOP = 8
D = 2048
FF = 512
LE = 32
CAP = 32
ALL = DEV * TOK
SLOTS = LE * CAP
CW = 512
NC = D // CW
GE = 8
NG = LE // GE
PIECES = NC * NG * 2
RING = 16
CW2 = 256
NC2 = D // CW2
HALF = TOK // 2
BF16_MAX = 3.3895313892515355e38


def kernel(tokens, ids, gates, w_in, w_out, out, tok, meta, meta_all, gsel, hid, core_in, x_in, y_in, z_in, ring, w_sem, t_sem, m_send, m_recv, a_send, a_recv, r_send, r_recv):
    y = lax.axis_index('row')
    col = lax.axis_index('col')
    x = col // 2
    k = col % 2
    g = y * 4 + col

    def place(dy, dx, dk):
        return (1 - y if dy else y), (1 - x if dx else x), (1 - k if dk else k)

    def dev(dy, dx, dk):
        yy, xx, kk = place(dy, dx, dk)
        return {'row': yy, 'col': xx * 2 + kk}

    def block(dy, dx, dk):
        yy, xx, kk = place(dy, dx, dk)
        return kk * 4 + xx * 2 + yy

    def rows(dy, dx, dk):
        return pl.ds(pl.multiple_of(block(dy, dx, dk) * TOK, TOK), TOK)

    def half_rows(dy, dx, dk, h):
        return pl.ds(pl.multiple_of(block(dy, dx, dk) * TOK + h * HALF, HALF), HALF)

    own = block(0, 0, 0)

    def tok_copy(c):
        return pltpu.make_async_copy(tokens.at[:, pl.ds(c * CW, CW)], tok.at[c, rows(0, 0, 0)], t_sem.at[c])

    for c in range(NC):
        tok_copy(c).start()

    def in_copy(p, slot):
        c, gr, half = p // (2 * NG), (p // 2) % NG, p % 2
        return pltpu.make_async_copy(
            w_in.at[pl.ds(gr * GE, GE), pl.ds(pl.multiple_of(c * CW, CW), CW), pl.ds(pl.multiple_of(half * 256, 256), 256)],
            ring.at[slot], w_sem.at[slot])

    def out_copy(p, slot):
        c, gr = p // NG, p % NG
        return pltpu.make_async_copy(
            w_out.at[pl.ds(gr * GE, GE), :, pl.ds(pl.multiple_of(c * CW2, CW2), CW2)], ring.at[slot], w_sem.at[slot])

    for p in range(RING):
        in_copy(p, p).start()

    def refill(p, slot):
        nxt = p + RING

        @pl.when(nxt < PIECES)
        def _():
            in_copy(nxt, slot).start()

        @pl.when(jnp.logical_and(nxt >= PIECES, nxt < 2 * PIECES))
        def _():
            out_copy(nxt - PIECES, slot).start()

    meta[0:TOP, :] = ids[...].astype(F32)
    meta[TOP:2 * TOP, :] = gates[...]

    rel = [(dy, dx, dk) for dy in (0, 1) for dx in (0, 1) for dk in (0, 1)]
    barrier = pltpu.get_barrier_semaphore()
    for r in rel[1:]:
        pl.semaphore_signal(barrier, inc=1, device_id=dev(*r), device_id_type=MESH)
    pl.semaphore_wait(barrier, DEV - 1)

    def meta_copy(i, dst):
        return pltpu.make_async_remote_copy(meta, meta_all.at[dst], m_send.at[i], m_recv.at[i], device_id=dev(*rel[i]),
                                            device_id_type=MESH)

    for i in range(1, DEV):
        meta_copy(i, own).start()

    def a_copy(c, i, region, to):
        ref = tok.at[c, region]
        return pltpu.make_async_remote_copy(ref, ref, a_send.at[c, i], a_recv.at[c, i], device_id=dev(*to), device_id_type=MESH)

    A_SENT = [((0, 0, 0), None, (0, 0, 1)), ((0, 0, 0), None, (0, 1, 0)), ((0, 0, 0), None, (1, 0, 0)),
              ((0, 1, 0), None, (0, 0, 1)), ((0, 1, 0), 0, (1, 0, 0)), ((1, 0, 0), None, (0, 0, 1)),
              ((1, 0, 0), 1, (0, 1, 0)), ((1, 1, 0), None, (0, 0, 1))]
    A_GOT = [((0, 0, 1), None), ((0, 1, 0), None), ((1, 0, 0), None), ((0, 1, 1), None), ((1, 1, 0), 0), ((1, 0, 1), None),
             ((1, 1, 0), 1), ((1, 1, 1), None)]

    def region(where, h):
        return rows(*where) if h is None else half_rows(*where, h)

    def a_start(c, i):
        where, h, to = A_SENT[i]
        a_copy(c, i, region(where, h), to).start()

    def a_wait_send(c, i):
        where, h, to = A_SENT[i]
        a_copy(c, i, region(where, h), to).wait_send()

    def a_wait(c, i):
        where, h = A_GOT[i]
        a_copy(c, i, region(where, h), A_SENT[i][2]).wait_recv()

    def a_own(c):
        tok_copy(c).wait()
        for i in (1, 2, 0):
            a_start(c, i)

    def a_forward(c):
        a_wait(c, 1)
        a_start(c, 4)
        a_start(c, 3)
        a_wait(c, 2)
        a_start(c, 6)
        a_start(c, 5)

    def a_corner(c):
        a_wait(c, 4)
        a_wait(c, 6)
        a_start(c, 7)

    a_own(0)
    a_own(1)

    def expert_rows(gr, i):
        return pl.ds(pl.multiple_of((gr * GE + i) * CAP, CAP), CAP)

    def gather_and_first(pos_t, lhs, expand, sel, buf, hacc):
        lane = lax.broadcasted_iota(jnp.int32, (TOK, SLOTS), 1)
        sub = lax.broadcasted_iota(jnp.int32, (TOK, SLOTS), 0)
        lane_expert = lax.shift_right_logical(lane, 5)
        for q in range(4):
            expand[q] = jnp.where(sub - LE * q == lane_expert, 1.0, 0.0).astype(BF16)
        hacc[...] = jnp.zeros_like(hacc)
        meta_all[own] = meta[...]

        for i in range(1, DEV):
            meta_copy(i, block(*rel[i])).wait_recv()

        eid = (g * LE + lax.broadcasted_iota(jnp.int32, (LE, 1), 0)).astype(F32)
        upper = jnp.where(lax.broadcasted_iota(jnp.int32, (TOK, TOK), 0) < lax.broadcasted_iota(jnp.int32, (TOK, TOK), 1), 1.0, 0.0)
        upper = upper.astype(BF16)
        before = jnp.zeros((LE, 1), F32)
        for gi in range(DEV):
            b = (gi % 2) * 4 + ((gi % 4) // 2) * 2 + gi // 4
            chose = jnp.zeros((LE, TOK), F32)
            gate = jnp.zeros((LE, TOK), F32)
            for j in range(TOP):
                hit = meta_all[b, j:j + 1, :] == eid
                chose = chose + jnp.where(hit, 1.0, 0.0)
                gate = gate + jnp.where(hit, meta_all[b, TOP + j:TOP + j + 1, :], 0.0)
            rank = jnp.dot(chose.astype(BF16), upper, preferred_element_type=F32) + before
            before = before + jnp.sum(chose, axis=1, keepdims=True)
            pos = jnp.where(jnp.logical_and(chose > 0.0, rank < float(CAP)), rank, -1.0)
            pos_t[:, b * TOK:(b + 1) * TOK] = pos
            high = jnp.minimum(gate, BF16_MAX).astype(BF16).astype(F32)
            rest = gate - high
            mid = rest.astype(BF16).astype(F32)
            low = rest - mid
            table = jnp.concatenate([pos, high, mid, low], axis=0)
            lhs[b * TOK:(b + 1) * TOK, :] = table.T.astype(BF16)

        a_forward(0)
        a_own(2)

        slot_rank = lax.broadcasted_iota(jnp.int32, (CAP, ALL), 0).astype(F32)

        def sel_step(e, _):
            row = pos_t[pl.ds(e, 1), :]
            sel[pl.ds(pl.multiple_of(e * CAP, CAP), CAP), :] = jnp.where(row == slot_rank, 1.0, 0.0).astype(BF16)
            return 0

        lax.fori_loop(0, LE, sel_step, 0)

        lane_rank = jnp.bitwise_and(lax.broadcasted_iota(jnp.int32, (TOK, SLOTS), 1), CAP - 1).astype(F32)

        def gate_step(b, _):
            rr = pl.ds(pl.multiple_of(b * TOK, TOK), TOK)
            table = lhs[rr, :]
            mine = jnp.dot(table, expand[0], preferred_element_type=F32) == lane_rank
            for q in range(3):
                val = jnp.dot(table, expand[q + 1], preferred_element_type=F32)
                gsel[q, rr, :] = jnp.where(mine, val, 0.0).astype(BF16)
            return 0

        lax.fori_loop(0, DEV // 2, gate_step, 0)
        a_forward(1)
        a_own(3)
        lax.fori_loop(DEV // 2, DEV, gate_step, 0)
        a_corner(0)

        def first_chunk(c, _):
            for i in (0, 3, 5, 7):
                a_wait(c, i)

            def dispatch(mb, _):
                rr = pl.ds(pl.multiple_of(mb * 256, 256), 256)
                buf[rr, :] = jnp.dot(sel[rr, :], tok[c], preferred_element_type=F32).astype(BF16)
                return 0

            lax.fori_loop(0, SLOTS // 256, dispatch, 0)

            def group(gr, _):
                @pl.when(jnp.logical_and(gr == 1, c + 2 < NC))
                def _():
                    a_forward(c + 2)

                @pl.when(jnp.logical_and(gr == 2, c + 1 < NC))
                def _():
                    a_corner(c + 1)

                p = (c * NG + gr) * 2
                slot = p % RING
                in_copy(p, slot).wait()
                in_copy(p + 1, slot + 1).wait()
                for i in range(GE):
                    rr = expert_rows(gr, i)
                    for h in range(2):
                        hacc[rr, h * 256:(h + 1) * 256] += jnp.dot(buf[rr, :], ring[slot + h, i], preferred_element_type=F32)
                refill(p, slot)
                refill(p + 1, slot + 1)
                return 0

            lax.fori_loop(0, NG, group, 0)
            return 0

        lax.fori_loop(0, NC, first_chunk, 0)

        def act(mb, _):
            rr = pl.ds(pl.multiple_of(mb * 128, 128), 128)
            hid[rr, :] = jax.nn.gelu(hacc[rr, :]).astype(BF16)
            return 0

        lax.fori_loop(0, SLOTS // 128, act, 0)

    pl.run_scoped(gather_and_first, pltpu.VMEM((LE, ALL), F32), pltpu.VMEM((ALL, TOK), BF16), pltpu.VMEM((4, TOK, SLOTS), BF16),
                  pltpu.VMEM((SLOTS, ALL), BF16), pltpu.VMEM((SLOTS, CW), BF16), pltpu.VMEM((SLOTS, FF), F32))

    def second_and_scatter(o_even, o_odd, part):
        def r_copy(c, i):
            src, dst, to = (
                (part.at[c, 1 - k], core_in.at[c], (0, 0, 1)),
                (part.at[c, k, 1 - x, :, 0], x_in.at[c], (0, 1, 0)),
                (part.at[c, k, :, 1 - y, 1], y_in.at[c], (1, 0, 0)),
                (part.at[c, k, x, 1 - y, 0], z_in.at[c, 0], (1, 0, 0)),
                (part.at[c, k, 1 - x, y, 1], z_in.at[c, 1], (0, 1, 0)),
            )[i]
            return pltpu.make_async_remote_copy(src, dst, r_send.at[c, i], r_recv.at[c, i], device_id=dev(*to), device_id_type=MESH)

        def r_first(c):
            r_copy(c, 0).wait_recv()

            def add(i, _):
                part[c, k, i] = part[c, k, i] + core_in[c, i]
                return 0

            lax.fori_loop(0, 2, add, 0)
            r_copy(c, 1).start()
            r_copy(c, 2).start()

        def r_second(c):
            r_copy(c, 1).wait_recv()
            part[c, k, x, 1 - y, 0] = part[c, k, x, 1 - y, 0] + x_in[c, 1 - y]
            r_copy(c, 3).start()
            r_copy(c, 2).wait_recv()
            part[c, k, 1 - x, y, 1] = part[c, k, 1 - x, y, 1] + y_in[c, 1 - x]
            r_copy(c, 4).start()

        def r_last(c):
            r_copy(c, 3).wait_recv()
            r_copy(c, 4).wait_recv()
            wide = c // 2
            cols = pl.ds(pl.multiple_of((c % 2) * CW2, CW2), CW2)
            for h in (0, 1):
                near = x_in[c, y] if h == 0 else y_in[c, x]
                total = part[c, k, x, y, h] + near + z_in[c, h]
                total = tok[wide, half_rows(0, 0, 0, h), cols].astype(F32) + total
                out[h * HALF:(h + 1) * HALF, pl.ds(pl.multiple_of(c * CW2, CW2), CW2)] = total.astype(BF16)

        def experts_out(c, gr, o_ref):
            q = c * NG + gr
            p = PIECES + q
            slot = p % RING
            for i in range(GE):
                rr = expert_rows(gr, i)
                o_ref[rr, :] = jnp.dot(hid[rr, :], ring[slot, i], preferred_element_type=F32).astype(BF16)

        def combine(c, gr, o_ref):
            core = (1 - k) + (gr // 2) * (2 * k - 1)
            mb = gr % 2
            rr = pl.ds(pl.multiple_of(core * 512 + mb * 256, 256), 256)
            o = o_ref[...]
            acc = jnp.dot(gsel[0, rr, :], o, preferred_element_type=F32)
            acc = acc + jnp.dot(gsel[1, rr, :], o, preferred_element_type=F32)
            acc = acc + jnp.dot(gsel[2, rr, :], o, preferred_element_type=F32)
            part[c, core, mb] = acc.reshape(2, 2, HALF, CW2)

        def ready(c, gr):
            q = c * NG + gr
            out_copy(q, (PIECES + q) % RING).wait()

        def free(c, gr):
            p = PIECES + c * NG + gr
            refill(p, p % RING)

        def handlers(c, gr):
            @pl.when(jnp.logical_and(gr == 1, c >= 1))
            def _():
                r_first(c - 1)

            @pl.when(gr == 2)
            def _():
                r_copy(c, 0).start()

            @pl.when(jnp.logical_and(gr == 3, c >= 3))
            def _():
                r_second(c - 3)

        def opening(gr, _):
            ready(0, gr)
            experts_out(0, gr, o_even)
            free(0, gr)
            return 0

        lax.fori_loop(0, NG, opening, 0)

        def both(c, o_here, o_next):
            def group(gr, _):
                handlers(c, gr)
                ready(c + 1, gr)
                combine(c, gr, o_here)
                experts_out(c + 1, gr, o_next)
                free(c + 1, gr)
                return 0

            lax.fori_loop(0, NG, group, 0)

        def pair(i, _):
            both(2 * i, o_even, o_odd)
            both(2 * i + 1, o_odd, o_even)
            return 0

        lax.fori_loop(0, NC2 // 2 - 1, pair, 0)
        both(NC2 - 2, o_even, o_odd)

        def closing(gr, _):
            handlers(NC2 - 1, gr)
            combine(NC2 - 1, gr, o_odd)
            return 0

        lax.fori_loop(0, NG, closing, 0)
        r_first(NC2 - 1)
        r_second(NC2 - 3)

        def finish(c, _):
            r_last(c)
            return 0

        lax.fori_loop(0, NC2 - 4, finish, 0)
        r_second(NC2 - 2)
        r_last(NC2 - 4)
        r_second(NC2 - 1)
        lax.fori_loop(NC2 - 3, NC2, finish, 0)

        def r_drain(c, _):
            for i in range(5):
                r_copy(c, i).wait_send()
            return 0

        lax.fori_loop(0, NC2, r_drain, 0)

    pl.run_scoped(second_and_scatter, pltpu.VMEM((SLOTS, CW2), BF16), pltpu.VMEM((SLOTS, CW2), BF16),
                  pltpu.VMEM((NC2, 2, 2, 2, 2, HALF, CW2), F32))

    for i in range(1, DEV):
        meta_copy(i, own).wait_send()

    def drain(c, _):
        for i in range(8):
            a_wait_send(c, i)
        return 0

    lax.fori_loop(0, NC, drain, 0)


def solution(mesh):
    def device_fn(tokens, expert_ids, gate_weights, w_in, w_out):
        dma = pltpu.SemaphoreType.DMA
        any_spec = pl.BlockSpec(memory_space=pl.ANY)
        vmem_spec = pl.BlockSpec(memory_space=pltpu.VMEM)
        return pl.pallas_call(
            kernel,
            out_shape=jax.ShapeDtypeStruct((TOK, D), BF16),
            in_specs=[any_spec, vmem_spec, vmem_spec, any_spec, any_spec],
            out_specs=vmem_spec,
            scratch_shapes=[
                pltpu.VMEM((NC, ALL, CW), BF16),
                pltpu.VMEM((2 * TOP, TOK), F32),
                pltpu.VMEM((DEV, 2 * TOP, TOK), F32),
                pltpu.VMEM((3, ALL, SLOTS), BF16),
                pltpu.VMEM((SLOTS, FF), BF16),
                pltpu.VMEM((NC2, 2, 2, 2, HALF, CW2), F32),
                pltpu.VMEM((NC2, 2, HALF, CW2), F32),
                pltpu.VMEM((NC2, 2, HALF, CW2), F32),
                pltpu.VMEM((NC2, 2, HALF, CW2), F32),
                pltpu.VMEM((RING, GE, 512, 256), BF16),
                dma((RING,)), dma((NC,)), dma((DEV,)), dma((DEV,)), dma((NC, 8)), dma((NC, 8)), dma((NC2, 5)), dma((NC2, 5)),
            ],
            compiler_params=pltpu.CompilerParams(collective_id=0, has_side_effects=True, vmem_limit_bytes=67043328),
            name='experts',
        )(tokens, expert_ids.T, gate_weights.T, w_in, w_out)

    token_spec = P(('data', 'row', 'col'), None)
    expert_spec = P(GRID_AXES, None, None)
    return jax.shard_map(device_fn, mesh=mesh, in_specs=(token_spec, token_spec, token_spec, expert_spec, expert_spec),
                         out_specs=token_spec, check_vma=False)
```
